256 devices in a mesh: leaf: 64 (over z, y, core), blk: 4 (over x).
Axes of the slice: x: 4, y: 4, z: 8, core: 2. Of those that a mesh axis runs over, the one named last changes fastest.
Arguments:
- src_pos: int32 [4, 16777216], P('blk', 'leaf'), may hold values from 0 to 67108863, as said below
- strengths: float32 [2, 4, 16777216], P(None, 'blk', 'leaf'), may hold values from -0.0007324219 to 0.0007324219
- tgt_pos: int32 [67108864], P(('leaf', 'blk')), may hold values from 0 to 201326591, as said below
Outputs:
- field: float32 [2, 67108864], P(None, ('leaf', 'blk'))
The draws below stay inside these ranges and needn't reach their ends.
Inputs may be any that keep to these rules, and one draw needn't show every extreme that they name: `src_pos`: row q holds 131072 runs of 128 cells; run b lies in the 128 cells from (q * 131072 + b) * 128 on. `tgt_pos`: the ticks held by index k of leaf, at every index of blk, come in 2048 runs of 128; run j lies in the 1536 ticks from (j * 64 + r) * 1536 on, where r is k with its 6 binary digits in reverse order.
All inputs are finite; a program needn't handle non-finite values.
Results may differ from the reference program's by a relative error of at most 0.0003.
Values sent between devices are 32-bit elements; how exact they have to be, the bound alone decides.
A program may use at most 128 MiB of HBM per device.

```python
import math
import jax
import jax.numpy as jnp
import numpy as np
from jax import lax

R = 16
PER_BOX = 128
TGT_BOX = 128
BOX_CELLS = 128
TOP_TICKS = 201326592
LB = 2048
GROUP_SRC = 16777216
N_LEAF = 64
N_BLK = 4


def draw_src_pos(key, part):
    column_count = N_LEAF * LB * PER_BOX
    row_ids = jnp.arange(N_BLK, dtype=jnp.int32)[:, None]
    columns = jnp.arange(column_count, dtype=jnp.int32)[None, :]
    box_ids = row_ids * (N_LEAF * LB) + columns // PER_BOX
    inside = jax.random.randint(jax.random.fold_in(key, 11), (N_BLK, column_count), 0, BOX_CELLS, dtype=jnp.int32)
    return box_ids * BOX_CELLS + inside


def draw_tgt_pos(key, part):
    per_device = LB * TGT_BOX
    flat_ids = jnp.arange(N_LEAF * N_BLK * per_device, dtype=jnp.int32)
    device = flat_ids // per_device
    leaf_no = device // N_BLK
    run_no = flat_ids % per_device // TGT_BOX
    bit_count = N_LEAF.bit_length() - 1
    reversed_leaf = jnp.zeros_like(leaf_no)
    for bit_no in range(bit_count):
        reversed_leaf = reversed_leaf * 2 + leaf_no // 2 ** bit_no % 2
    box_ticks = TOP_TICKS // (LB * N_LEAF)
    box_ids = run_no * N_LEAF + reversed_leaf
    inside = jax.random.randint(jax.random.fold_in(key, 23), flat_ids.shape, 0, box_ticks, dtype=jnp.int32)
    return box_ids * box_ticks + inside


def level_of(rng, extent, cuts, low, largest):
    def one(position, shards_of):
        heights = jax.random.uniform(jax.random.fold_in(jax.random.fold_in(rng, 6), position), (shards_of,), jnp.float32, low / len(cuts), largest / len(cuts))
        return jnp.repeat(jnp.exp(heights), extent[position] // shards_of).reshape((-1,) + (1,) * (len(extent) - position - 1))

    factor_of = one(*cuts[0])
    for cut in cuts[1:]:
        factor_of = factor_of * one(*cut)
    return factor_of


def gaussian(rng, dims, scale, most, shards=(), kind=jnp.bfloat16):
    drawn = scale * jax.random.normal(rng, dims, jnp.float32)
    if shards:
        drawn = drawn * level_of(rng, dims, shards, -0.22, 0.18)
    return jnp.clip(drawn, -most, most).astype(kind)


def setup_inputs(seed: int = 0) -> dict:
    splits = jax.random.split(jax.random.key(seed), 4)
    src_pos = draw_src_pos(jax.random.fold_in(splits[3], 71), 0)
    strengths = gaussian(splits[1], (2, N_BLK, GROUP_SRC), (N_BLK * GROUP_SRC) ** -0.5, 0.0007324219, ((1, 4), (2, 64)), jnp.float32)
    tgt_pos = draw_tgt_pos(jax.random.fold_in(splits[3], 71), 0)
    return {"src_pos": src_pos, "strengths": strengths, "tgt_pos": tgt_pos}


highest_accuracy = lax.Precision.HIGHEST


def node_offsets(box_cells):
    node_index = np.arange(R)
    unit_nodes = (1.0 - np.cos(np.pi * (node_index + 0.5) / R)) / 2.0
    return np.floor(box_cells * unit_nodes).astype(np.int64)


def lagrange_values(node_pos, points):
    basis_rows = []
    for row_node in range(node_pos.shape[0]):
        column = np.ones(points.shape[0])
        for other_node in range(node_pos.shape[0]):
            if other_node != row_node:
                column = column * (points - node_pos[other_node]) / (node_pos[row_node] - node_pos[other_node])
        basis_rows.append(column)
    return np.stack(basis_rows)


def turn_angle(tick_ids, cell_index_list):
    product = tick_ids * cell_index_list
    return product.astype(jnp.float32) * (2.0 * math.pi / 2.0 ** 32)


def leaf_weights(in_box, amounts):
    box_count = in_box.shape[0]
    block_size = min(box_count, 512)
    center = TOP_TICKS // 2
    leaf_nodes = node_offsets(BOX_CELLS)
    node_angles = np.pi * (np.arange(R) + 0.5) / R
    exact_nodes = np.cos(node_angles)
    at_exact = lagrange_values(2.0 * leaf_nodes / BOX_CELLS - 1.0, exact_nodes)
    cheb_at = np.stack([np.cos(degree * node_angles) for degree in range(R)])
    norm_weights = np.where(np.arange(R) == 0, 1.0, 2.0) / R
    coefficients = jnp.asarray(norm_weights[:, None] * (cheb_at @ at_exact.T), jnp.float32)

    def one_block(block_no):
        box_part = lax.dynamic_slice_in_dim(in_box, block_no * block_size, block_size, 0)
        strength_blk = lax.dynamic_slice_in_dim(amounts, block_no * block_size, block_size, 1)
        angles = turn_angle(jnp.int32(center), box_part)
        rotate_re = jnp.cos(angles)
        rotation_imaginary = jnp.sin(angles)
        source_re = rotate_re * strength_blk[0] - rotation_imaginary * strength_blk[1]
        source_im = rotation_imaginary * strength_blk[0] + rotate_re * strength_blk[1]
        scaled = box_part.astype(jnp.float32) * (2.0 / BOX_CELLS) - 1.0
        chebyshev = [jnp.ones_like(scaled), scaled]
        for degree in range(2, R):
            chebyshev.append(2.0 * scaled * chebyshev[-1] - chebyshev[-2])
        moments = jnp.einsum('nbk,xbk->xnb', jnp.stack(chebyshev), jnp.stack([source_re, source_im]), precision=highest_accuracy)
        return jnp.einsum('nt,xnb->xtb', coefficients, moments, precision=highest_accuracy)

    blocks = lax.map(one_block, jnp.arange(box_count // block_size, dtype=jnp.int32))
    mixed_nodes = jnp.transpose(blocks, (1, 2, 0, 3)).reshape(2, R, box_count)
    post_turn = turn_angle(jnp.int32(center), jnp.asarray(leaf_nodes, jnp.int32))
    post_re = jnp.cos(post_turn)[:, None]
    post_im = jnp.sin(post_turn)[:, None]
    out_re = post_re * mixed_nodes[0] + post_im * mixed_nodes[1]
    out_im = post_re * mixed_nodes[1] - post_im * mixed_nodes[0]
    return jnp.stack([out_re, out_im]).reshape(2, R, 1, box_count)


def parent_level(paired, child_ids, tree_level):
    box_a = child_ids.shape[0]
    box_e = child_ids.shape[1]
    box_s = paired.shape[3]
    child_cells = BOX_CELLS * 2 ** tree_level
    child_nodes = node_offsets(child_cells)
    parent_nodes = node_offsets(2 * child_cells)
    inner_cells = np.concatenate([child_nodes, child_nodes + child_cells])
    blend_matrix = jnp.asarray(lagrange_values(parent_nodes / (2.0 * child_cells), inner_cells / (2.0 * child_cells)).reshape(R, 2, R), jnp.float32)
    box_ticks = TOP_TICKS // 2 ** (tree_level + 1)
    centers = child_ids * box_ticks + box_ticks // 2
    pre_turn = turn_angle(centers[:, :, None], jnp.asarray(inner_cells, jnp.int32)[None, None, :]).reshape(box_a, box_e, 2, R)
    pre_re = jnp.cos(pre_turn)[..., None]
    pre_im = jnp.sin(pre_turn)[..., None]
    source = jnp.transpose(paired, (0, 2, 4, 1, 3))[:, :, None]
    rotated_real = pre_re * source[0] - pre_im * source[1]
    rotated_imaginary = pre_im * source[0] + pre_re * source[1]
    accumulated_sum = jnp.einsum('jiw,fpziwd->fjpzd', blend_matrix, jnp.stack([rotated_real, rotated_imaginary]), precision=highest_accuracy)
    post_turn = turn_angle(centers[:, :, None], jnp.asarray(parent_nodes, jnp.int32)[None, None, :])
    post_re = jnp.transpose(jnp.cos(post_turn), (2, 0, 1))[:, :, :, None]
    post_im = jnp.transpose(jnp.sin(post_turn), (2, 0, 1))[:, :, :, None]
    out_re = post_re * accumulated_sum[0] + post_im * accumulated_sum[1]
    out_im = post_re * accumulated_sum[1] - post_im * accumulated_sum[0]
    return jnp.stack([out_re, out_im]).reshape(2, R, box_a * box_e, box_s)


def tree_up(weights, tree_level, first_box):
    box_a = weights.shape[2]
    box_s = weights.shape[3]
    paired = weights.reshape(2, R, box_a, box_s // 2, 2)
    parents = first_box + jnp.arange(box_a, dtype=jnp.int32)
    child_ids = 2 * parents[:, None] + jnp.arange(2, dtype=jnp.int32)[None, :]
    return parent_level(paired, child_ids, tree_level)


def reference(src_pos, strengths, tgt_pos):
    block_count = src_pos.shape[0]
    group_boxes = src_pos.shape[1] // PER_BOX
    tree_depth = group_boxes.bit_length() - 1
    group_cells = group_boxes * BOX_CELLS
    root_list = []
    for source_blk in range(block_count):
        in_box = (src_pos[source_blk] % BOX_CELLS).reshape(group_boxes, PER_BOX)
        amounts = strengths[:, source_blk].reshape(2, group_boxes, PER_BOX)
        weights = leaf_weights(in_box, amounts)
        for tree_level in range(tree_depth):
            weights = tree_up(weights, tree_level, 0)
        root_list.append(weights.reshape(2, R, group_boxes))
    root_sets = jnp.stack(root_list)
    top_nodes = jnp.asarray(node_offsets(group_cells), jnp.int32)
    final_ticks = TOP_TICKS // group_boxes
    target_count = tgt_pos.shape[0]
    block_size = min(target_count, 65536)

    def one_block(block_no):
        ticks_blk = lax.dynamic_slice_in_dim(tgt_pos, block_no * block_size, block_size, 0)
        box_ids = ticks_blk // final_ticks
        picked = jnp.take(root_sets, box_ids, axis=3)
        angles = turn_angle(ticks_blk[None, :], top_nodes[:, None])
        phase_re = jnp.cos(angles)
        phase_im = jnp.sin(angles)
        field_re = jnp.zeros(ticks_blk.shape, jnp.float32)
        field_imaginary = jnp.zeros(ticks_blk.shape, jnp.float32)
        for source_blk in range(block_count):
            part_re = picked[source_blk, 0]
            part_im = picked[source_blk, 1]
            inner_re = jnp.sum(phase_re * part_re - phase_im * part_im, axis=0)
            inner_im = jnp.sum(phase_re * part_im + phase_im * part_re, axis=0)
            outer_turn = turn_angle(ticks_blk, jnp.int32(source_blk * group_cells))
            outer_re = jnp.cos(outer_turn)
            outer_im = jnp.sin(outer_turn)
            field_re = field_re + outer_re * inner_re - outer_im * inner_im
            field_imaginary = field_imaginary + outer_re * inner_im + outer_im * inner_re
        return jnp.stack([field_re, field_imaginary])

    blocks = lax.map(one_block, jnp.arange(target_count // block_size, dtype=jnp.int32))
    return jnp.transpose(blocks, (1, 0, 2)).reshape(2, target_count)
```

```python
import functools
import math

import jax
import jax.numpy as jnp
import numpy as np
from jax import lax
from jax.experimental import pallas as pl
from jax.experimental.pallas import tpu as pltpu
from jax.sharding import PartitionSpec as P

R = 16
CELLS = 128
TOP_TICKS = 201326592
BOX_TICKS = 1536
HALF = BOX_TICKS // 2
N_BLK = 4
MESH = pl.DeviceIdType.MESH


def node_offsets(box_cells):
    unit = (1.0 - np.cos(np.pi * (np.arange(R) + 0.5) / R)) / 2.0
    return np.floor(box_cells * unit).astype(np.int64)


def lagrange_values(node_pos, points):
    rows = []
    for a in range(node_pos.shape[0]):
        col = np.ones(points.shape[0])
        for b in range(node_pos.shape[0]):
            if b != a:
                col = col * (points - node_pos[b]) / (node_pos[a] - node_pos[b])
        rows.append(col)
    return np.stack(rows)


def phase(ticks, cells):
    product = (int(ticks) * np.asarray(cells, np.int64)) % (1 << 32)
    return np.exp(2j * np.pi * product / 2.0**32)


def level_matrix(level):
    cells = CELLS << level
    child, parent = node_offsets(cells), node_offsets(2 * cells)
    inner = np.concatenate([child, child + cells])
    blend = lagrange_values(parent / (2.0 * cells), inner / (2.0 * cells))
    blend = blend.astype(np.float32).astype(np.float64).reshape(R, 2, R)
    signed = blend * np.array([1.0, -1.0])[None, :, None]
    quarter = (TOP_TICKS >> level) // 4
    sides = [phase(-quarter, child), phase(quarter, child)]
    return np.stack([signed * side[None, None, :] for side in sides])


def stage_complex(first, count):
    out = np.eye(R, dtype=np.complex128).reshape(1, R, 1, R)
    for level in range(first, first + count):
        step = level_matrix(level)
        joined = np.einsum("etju,aubs->aetjbs", step, out)
        n = out.shape[0]
        out = joined.reshape(2 * n, R, 2 * n, R)
    return out


def real_form(mat):
    n, m = mat.shape[0], mat.shape[2]
    out = np.zeros((n, 2, R, m, 2, R))
    out[:, 0, :, :, 0] = mat.real
    out[:, 0, :, :, 1] = -mat.imag
    out[:, 1, :, :, 0] = mat.imag
    out[:, 1, :, :, 1] = mat.real
    return out.reshape(n * 2 * R, m * 2 * R)


def leaf_map():
    nodes = node_offsets(CELLS)
    angles = np.pi * (np.arange(R) + 0.5) / R
    at_exact = lagrange_values(2.0 * nodes / CELLS - 1.0, np.cos(angles))
    cheb = np.stack([np.cos(n * angles) for n in range(R)])
    norm = np.where(np.arange(R) == 0, 1.0, 2.0) / R
    coef = (norm[:, None] * (cheb @ at_exact.T)).astype(np.float32).astype(np.float64)
    split = np.zeros((R, R))
    for n in range(8):
        split[n, n] = 1.0
    split[8, 8] = 1.0
    for i in range(1, 8):
        split[8 + i, 8 + i] = 2.0
        split[8 + i, 8 - i] -= 1.0
    return coef.T @ split


def stage_tables():
    mats = []
    leaf = leaf_map()
    first = stage_complex(0, 3)
    mats.append(real_form(np.einsum("atbs,sn->atbn", first, leaf)))
    mats.append(real_form(stage_complex(3, 3)))
    mats.append(real_form(stage_complex(6, 3)))
    two = stage_complex(9, 2)
    wide = np.einsum("atbs,ij->aitbjs", two, np.eye(2)).reshape(8, R, 8, R)
    mats.append(real_form(wide))
    mats.append(real_form(stage_complex(11, 3)))
    mats.append(real_form(stage_complex(14, 3)))
    return np.stack(mats)


def top_frequency():
    nodes = node_offsets(CELLS << 17)
    q = np.arange(N_BLK)[:, None]
    return nodes, nodes[None, :] / 2.0**32 + q / 256.0


def hi_lo(table):
    full = np.asarray(table, np.float32)
    hi = full.astype(jnp.bfloat16)
    lo = (full - hi.astype(np.float32)).astype(jnp.bfloat16)
    return hi, lo


@functools.lru_cache(None)
def tables():
    hi, lo = hi_lo(stage_tables())
    stages = np.stack([hi, lo], axis=1)
    nodes, freq = top_frequency()
    y = np.arange(HALF) + 0.5
    angle = 2.0 * np.pi * ((freq.reshape(-1)[:, None] * y[None, :]) % 1.0)
    wave_hi, wave_lo = hi_lo(np.concatenate([np.cos(angle), np.sin(angle)], axis=1))
    waves = np.concatenate([wave_hi, wave_hi, wave_lo, wave_lo], axis=0)
    q = np.arange(N_BLK)[:, None]
    shift = np.exp(2j * np.pi * ((-0.5 * nodes[None, :] / 2.0**32 + q * (HALF - 0.5) / 256.0) % 1.0))
    shift = np.concatenate([shift.real, shift.imag], axis=1).astype(np.float32)
    shift = np.broadcast_to(shift[:, :, None], (N_BLK, 2 * R, 128)).copy()
    turns = (3 * np.arange(CELLS)) % CELLS / CELLS
    spin = np.stack([np.cos(2 * np.pi * turns), np.sin(2 * np.pi * turns)]).astype(np.float32)
    spin = np.broadcast_to(spin[:, None, :], (2, 8, CELLS)).copy()
    return stages, waves, shift, spin


def swap_lane(blocks, row_bit, lane_bit):
    out = list(blocks)
    amount = 1 << lane_bit
    for i in range(len(blocks)):
        if i >> row_bit & 1:
            continue
        k = i | 1 << row_bit
        x0, x1 = blocks[i], blocks[k]
        mask = (lax.broadcasted_iota(jnp.int32, x0.shape, 1) & amount) != 0
        out[i] = jnp.where(mask, pltpu.roll(x1, amount, 1), x0)
        out[k] = jnp.where(mask, x1, pltpu.roll(x0, 128 - amount, 1))
    return out


def swap_half(left, right, row_bit):
    left, right = list(left), list(right)
    for i in range(len(left)):
        if i >> row_bit & 1:
            continue
        k = i | 1 << row_bit
        left[k], right[i] = right[i], left[k]
    return left, right


def gather_rows(blocks):
    return jnp.concatenate(blocks, axis=0)


def split_rows(x, rows):
    return [x[i * rows : (i + 1) * rows] for i in range(x.shape[0] // rows)]


def apply_stage(stage_ref, index, left, right):
    x = jnp.concatenate([left, right], axis=1)
    hi = x.astype(jnp.bfloat16)
    lo = (x - hi.astype(jnp.float32)).astype(jnp.bfloat16)
    w_hi, w_lo = stage_ref[index, 0], stage_ref[index, 1]
    dot = functools.partial(jnp.dot, preferred_element_type=jnp.float32)
    y = dot(w_hi, hi) + (dot(w_lo, hi) + dot(w_hi, lo))
    return y[:, :128], y[:, 128:]


LAG = 2


def leaf_sums(pos, amp, spin_re, spin_im, mom, half):
    def beta_step(beta, carry):
        cells, amp_re, amp_im = [], [], []
        for group in range(16):
            s7, s6, s10, s9 = group >> 3 & 1, group >> 2 & 1, group >> 1 & 1, group & 1
            slab, rows = s10 * 2 + s9, pl.ds(beta + s6 * 64 + s7 * 128, 8, stride=8)
            cell = pos[slab, half, rows, :] & (CELLS - 1)
            sr, si = amp[0, slab, half, rows, :], amp[1, slab, half, rows, :]
            wr = jnp.take_along_axis(spin_re, cell, axis=1)
            wi = jnp.take_along_axis(spin_im, cell, axis=1)
            cells.append(cell.astype(jnp.float32) * (2.0 / CELLS) - 1.0)
            amp_re.append(wr * sr - wi * si)
            amp_im.append(wi * sr + wr * si)
        v_all = jnp.concatenate(cells, axis=0).T
        re_all = jnp.concatenate(amp_re, axis=0).T
        im_all = jnp.concatenate(amp_im, axis=0).T
        acc = [None] * 32
        for step in range(16):
            rows = slice(step * 8, step * 8 + 8)
            v, sr, si = v_all[rows], re_all[rows], im_all[rows]
            cheb = [None, v]
            twice = v + v
            cheb.append(twice * v - 1.0)
            for n in range(3, 9):
                cheb.append(twice * cheb[-1] - cheb[-2])
            for side, (a, b) in enumerate(((sr, si), (cheb[8] * sr, cheb[8] * si))):
                for n in range(8):
                    pa = a if n == 0 else cheb[n] * a
                    pb = b if n == 0 else cheb[n] * b
                    ia, ib = side * 8 + n, 16 + side * 8 + n
                    acc[ia] = pa if acc[ia] is None else acc[ia] + pa
                    acc[ib] = pb if acc[ib] is None else acc[ib] + pb
        for n in range(32):
            mom[beta, n : n + 1, half * 128 : half * 128 + 128] = jnp.sum(acc[n], axis=0, keepdims=True)
        return carry

    lax.fori_loop(0, 8, beta_step, 0)


def lane_swaps(x, pairs):
    blocks = split_rows(x, 32)
    for row_bit, lane_bit in pairs:
        blocks = swap_lane(blocks, row_bit, lane_bit)
    return blocks


def local_tree(stage, mom, out):
    sums = mom[...].reshape(256, 256)
    left, right = apply_stage(stage, 0, sums[:, :128], sums[:, 128:])
    pairs = ((2, 2), (1, 1), (0, 0))
    left, right = apply_stage(
        stage, 1, gather_rows(lane_swaps(left, pairs)), gather_rows(lane_swaps(right, pairs))
    )
    pairs = ((1, 6), (0, 5))
    left, right = swap_half(lane_swaps(left, pairs), lane_swaps(right, pairs), 2)
    left, right = apply_stage(stage, 2, gather_rows(left), gather_rows(right))
    pairs = ((2, 4), (1, 3), (0, 2))
    left, right = apply_stage(
        stage, 3, gather_rows(lane_swaps(left, pairs)), gather_rows(lane_swaps(right, pairs))
    )
    for half, x in enumerate((left, right)):
        tiles = split_rows(x, 8)
        tiles = swap_lane(swap_lane(tiles, 1, 1), 0, 0)
        for i in range(32):
            e9, e10, e0, e1, e2 = i >> 4 & 1, i >> 3 & 1, i >> 2 & 1, i >> 1 & 1, i & 1
            out[e0 * 32 + e1 * 16 + e2 * 8 + e9 * 4 + e10 * 2 + half] = tiles[i]


def cross_tree(stage, shift, got, out):
    halves = []
    for half in range(2):
        tiles = [None] * 32
        for d in range(32):
            tiles[(d & 7) * 4 + (d >> 4 & 1) * 2 + (d >> 3 & 1)] = got[half * 32 + d]
        halves.append(swap_lane(swap_lane(tiles, 1, 1), 0, 0))
    left, right = apply_stage(stage, 4, gather_rows(halves[0]), gather_rows(halves[1]))
    pairs = ((1, 1), (0, 0))
    left, right = swap_half(lane_swaps(left, pairs), lane_swaps(right, pairs), 2)
    left, right = apply_stage(stage, 5, gather_rows(left), gather_rows(right))
    shift_re, shift_im = shift[:R], shift[R:]
    for half, x in enumerate((left, right)):
        turned = []
        for block in split_rows(x, 32):
            re, im = block[:R], block[R:]
            turned.append(shift_re * re - shift_im * im)
            turned.append(shift_im * re + shift_re * im)
        tiles = split_rows(gather_rows(turned), 8)
        tiles = swap_lane(swap_lane(tiles, 1, 1), 0, 0)
        for i in range(32):
            e14, e15, e16, e12, e13 = i >> 4 & 1, i >> 3 & 1, i >> 2 & 1, i >> 1 & 1, i & 1
            out[half + e12 * 2 + e13 * 4 + e14 * 8 + e15 * 16 + e16 * 32] = tiles[i]


def coefficients(roots, z):
    parts = [[], []]
    for q in range(N_BLK):
        for half in range(2):
            tiles = [roots[q, z * 8 + (c * 2 + half)] for c in range(4)]
            parts[half].append(swap_lane(swap_lane(tiles, 1, 1), 0, 0))
    out = []
    for half in range(2):
        sides = []
        for c in range(2):
            rows = []
            for q in range(N_BLK):
                rows += parts[half][q][2 * c : 2 * c + 2]
            x = jnp.concatenate(rows, axis=0)
            hi = x.astype(jnp.bfloat16).astype(jnp.float32)
            t = jnp.concatenate([hi, x - hi], axis=0).T.astype(jnp.bfloat16)
            sides.append(jnp.concatenate([t, t], axis=1))
        out.append(sides)
    return out


def look_up(dense, tick, out, z, half, reverse):
    sub = lax.broadcasted_iota(jnp.int32, (8, 128), 0)
    for i in range(16):
        row = i * 8
        base = z * 256 + (half * 128 + row)
        y = tick[pl.ds(base, 8), :] - ((base + sub) * 64 + reverse) * BOX_TICKS - HALF
        upper = y >= 0
        index = jnp.where(upper, y, -1 - y)
        low, high = index & 127, index >> 7
        sums = [None] * 4
        for h in range(6):
            pick = high == h
            for c in range(2):
                for part in range(2):
                    start = part * HALF + h * 128
                    got = jnp.take_along_axis(dense[c, row : row + 8, start : start + 128], low, axis=1)
                    k = c * 2 + part
                    sums[k] = got if h == 0 else jnp.where(pick, got, sums[k])
        re_even, re_odd, im_even, im_odd = sums
        re_odd = jnp.where(upper, re_odd, -re_odd)
        im_odd = jnp.where(upper, im_odd, -im_odd)
        out[pl.ds(base * 2, 8, stride=2), :] = re_even - im_odd
        out[pl.ds(base * 2 + 1, 8, stride=2), :] = im_even + re_odd


def kernel(
    pos_in, amp_in, tick_in, stage_in, wave_in, shift_in, spin_in, out_hbm,
    pos, amp, tick, stage, wave, shift, spin, mom,
    first_src, first_dst, second_src, roots, out, dense0, dense1,
    load_sem, store_sem, send1, recv1, send2, recv2, send3, recv3,
):
    leaf, blk = lax.axis_index("leaf"), lax.axis_index("blk")
    own_z = leaf // 8

    loads = [
        pltpu.make_async_copy(spin_in, spin, load_sem.at[0]),
        pltpu.make_async_copy(pos_in.at[:, 0], pos.at[:, 0], load_sem.at[1]),
        pltpu.make_async_copy(amp_in.at[:, :, 0], amp.at[:, :, 0], load_sem.at[2]),
        pltpu.make_async_copy(pos_in.at[:, 1], pos.at[:, 1], load_sem.at[3]),
        pltpu.make_async_copy(amp_in.at[:, :, 1], amp.at[:, :, 1], load_sem.at[4]),
        pltpu.make_async_copy(stage_in, stage, load_sem.at[5]),
        pltpu.make_async_copy(shift_in.at[blk], shift, load_sem.at[6]),
        pltpu.make_async_copy(wave_in, wave, load_sem.at[7]),
        pltpu.make_async_copy(tick_in, tick, load_sem.at[8]),
    ]
    for load in loads:
        load.start()
    barrier = pltpu.get_barrier_semaphore()

    def greet(i, carry):
        pl.semaphore_signal(barrier, inc=1, device_id={"leaf": leaf ^ i}, device_id_type=MESH)
        return carry

    lax.fori_loop(1, 64, greet, 0)
    for i in range(1, N_BLK):
        pl.semaphore_signal(barrier, inc=1, device_id={"blk": (blk + i) % N_BLK}, device_id_type=MESH)

    for load in loads[:3]:
        load.wait()
    spin_re, spin_im = spin[0], spin[1]
    leaf_sums(pos, amp, spin_re, spin_im, mom, 0)
    for load in loads[3:5]:
        load.wait()
    leaf_sums(pos, amp, spin_re, spin_im, mom, 1)
    loads[5].wait()
    local_tree(stage, mom, first_src)
    pl.semaphore_wait(barrier, 63 + N_BLK - 1)

    def first(i):
        return pltpu.make_async_remote_copy(
            src_ref=first_src.at[leaf ^ i],
            dst_ref=first_dst.at[leaf],
            send_sem=send1.at[i],
            recv_sem=recv1.at[i],
            device_id={"leaf": leaf ^ i},
            device_id_type=MESH,
        )

    def first_send(i, carry):
        first(i).start()
        return carry

    def first_wait(i, carry):
        first(i).wait()
        return carry

    lax.fori_loop(1, 64, first_send, 0)
    first_dst[leaf] = first_src[leaf]
    loads[6].wait()
    lax.fori_loop(1, 64, first_wait, 0)
    cross_tree(stage, shift[...], first_dst, second_src)

    def near_z(c):
        k = (c + 1) // 2
        return (own_z + k * (2 * (c % 2) - 1) + 8) % 8

    def second(c, j):
        other = near_z(c) * 8 + j
        return pltpu.make_async_remote_copy(
            src_ref=second_src.at[other],
            dst_ref=roots.at[blk, leaf],
            send_sem=send2.at[other],
            recv_sem=recv2.at[leaf],
            device_id={"leaf": other},
            device_id_type=MESH,
        )

    def second_got(z, j):
        other = z * 8 + j
        return pltpu.make_async_remote_copy(
            src_ref=second_src.at[other],
            dst_ref=roots.at[blk, other],
            send_sem=send2.at[other],
            recv_sem=recv2.at[other],
            device_id={"leaf": other},
            device_id_type=MESH,
        )

    own_j = leaf % 8

    def send_own(i, carry):
        second(0, (own_j + i) % 8).start()
        return carry

    lax.fori_loop(1, 8, send_own, 0)

    def send_far(n, carry):
        second(n // 8, (own_j + n) % 8).start()
        return carry

    lax.fori_loop(8, 64, send_far, 0)
    roots[blk, leaf] = second_src[leaf]
    loads[7].wait()
    loads[8].wait()

    def third(z, i):
        return pltpu.make_async_remote_copy(
            src_ref=roots.at[blk, pl.ds(z * 8, 8)],
            dst_ref=roots.at[blk, pl.ds(z * 8, 8)],
            send_sem=send3.at[z, i],
            recv_sem=recv3.at[z, i],
            device_id={"blk": (blk + i) % N_BLK},
            device_id_type=MESH,
        )

    def third_got(z, i):
        source = (blk + N_BLK - i) % N_BLK
        return pltpu.make_async_remote_copy(
            src_ref=roots.at[blk, pl.ds(z * 8, 8)],
            dst_ref=roots.at[source, pl.ds(z * 8, 8)],
            send_sem=send3.at[z, i],
            recv_sem=recv3.at[z, i],
            device_id={"blk": (blk + i) % N_BLK},
            device_id_type=MESH,
        )

    def store(z):
        return pltpu.make_async_copy(
            out.at[pl.ds(z * 512, 512)], out_hbm.at[pl.ds(z * 512, 512)], store_sem.at[z]
        )

    reverse = jnp.int32(0)
    for bit in range(6):
        reverse = reverse * 2 + (leaf // 2**bit) % 2

    def chunk_step(c, carry):
        @pl.when(c < 8)
        def _():
            z = near_z(c)

            def got(j, carry):
                second_got(z, (own_j + j) % 8).wait_recv()
                return carry

            lax.fori_loop(jnp.where(c == 0, 1, 0), 8, got, 0)
            for i in (2, 1, 3):
                third(z, i).start()

        @pl.when(c >= LAG)
        def _():
            z = near_z(c - LAG)
            for i in (1, 2, 3):
                third_got(z, i).wait_recv()
            lhs = coefficients(roots, z)
            for half, dense in enumerate((dense0, dense1)):
                for side in range(2):
                    dense[side] = jnp.dot(lhs[half][side], wave[...], preferred_element_type=jnp.float32)
            for half, dense in enumerate((dense0, dense1)):
                look_up(dense, tick, out, z, half, reverse)
            store(z).start()

        return carry

    lax.fori_loop(0, 8 + LAG, chunk_step, 0)

    def finish(z, carry):
        store(z).wait()
        for i in (1, 2, 3):
            third(z, i).wait_send()
        return carry

    lax.fori_loop(0, 8, finish, 0)

    def finish_second(i, carry):
        second_got(0, leaf ^ i).wait_send()
        return carry

    lax.fori_loop(1, 64, finish_second, 0)


def local(src_pos, strengths, tgt_pos):
    stages, waves, shift, spin = tables()
    hbm = pl.BlockSpec(memory_space=pl.ANY)
    vmem, dma = pltpu.VMEM, pltpu.SemaphoreType.DMA
    f32, tiles = jnp.float32, (64, 8, 128)
    out = pl.pallas_call(
        kernel,
        out_shape=jax.ShapeDtypeStruct((4096, 128), f32),
        in_specs=[hbm] * 7,
        out_specs=hbm,
        scratch_shapes=[
            vmem((4, 2, 256, 128), jnp.int32),
            vmem((2, 4, 2, 256, 128), f32),
            vmem((2048, 128), jnp.int32),
            vmem((6, 2, 256, 256), jnp.bfloat16),
            vmem((256, 2 * HALF), jnp.bfloat16),
            vmem((2 * R, 128), f32),
            vmem((2, 8, 128), f32),
            vmem((8, 32, 256), f32),
            vmem(tiles, f32),
            vmem(tiles, f32),
            vmem(tiles, f32),
            vmem((N_BLK, *tiles), f32),
            vmem((4096, 128), f32),
            vmem((2, 128, 2 * HALF), f32),
            vmem((2, 128, 2 * HALF), f32),
            dma((9,)),
            dma((8,)),
            dma((64,)),
            dma((64,)),
            dma((64,)),
            dma((64,)),
            dma((8, N_BLK)),
            dma((8, N_BLK)),
        ],
        compiler_params=pltpu.CompilerParams(collective_id=0, has_side_effects=True),
        name="butterfly",
    )(
        src_pos.reshape(4, 2, 256, 128),
        strengths.reshape(2, 4, 2, 256, 128),
        tgt_pos.reshape(2048, 128),
        jnp.asarray(stages),
        jnp.asarray(waves),
        jnp.asarray(shift),
        jnp.asarray(spin),
    )
    return jnp.transpose(out.reshape(2048, 2, 128), (1, 0, 2)).reshape(2, 2048 * 128)


def solution(mesh):
    return jax.shard_map(
        local,
        mesh=mesh,
        in_specs=(P("blk", "leaf"), P(None, "blk", "leaf"), P(("leaf", "blk"))),
        out_specs=P(None, ("leaf", "blk")),
        check_vma=False,
    )
```

```python
import functools
import math

import jax
import jax.numpy as jnp
import numpy as np
from jax import lax
from jax.experimental import pallas as pl
from jax.experimental.pallas import tpu as pltpu
from jax.sharding import PartitionSpec as P

R = 16
CELLS = 128
TOP_TICKS = 201326592
BOX_TICKS = 1536
HALF = BOX_TICKS // 2
N_BLK = 4
MESH = pl.DeviceIdType.MESH
SPAN = 32000.0


def node_offsets(box_cells):
    unit = (1.0 - np.cos(np.pi * (np.arange(R) + 0.5) / R)) / 2.0
    return np.floor(box_cells * unit).astype(np.int64)


def lagrange_values(node_pos, points):
    rows = []
    for a in range(node_pos.shape[0]):
        col = np.ones(points.shape[0])
        for b in range(node_pos.shape[0]):
            if b != a:
                col = col * (points - node_pos[b]) / (node_pos[a] - node_pos[b])
        rows.append(col)
    return np.stack(rows)


def phase(ticks, cells):
    product = (int(ticks) * np.asarray(cells, np.int64)) % (1 << 32)
    return np.exp(2j * np.pi * product / 2.0**32)


def level_matrix(level):
    cells = CELLS << level
    child, parent = node_offsets(cells), node_offsets(2 * cells)
    inner = np.concatenate([child, child + cells])
    blend = lagrange_values(parent / (2.0 * cells), inner / (2.0 * cells))
    blend = blend.astype(np.float32).astype(np.float64).reshape(R, 2, R)
    signed = blend * np.array([1.0, -1.0])[None, :, None]
    quarter = (TOP_TICKS >> level) // 4
    sides = [phase(-quarter, child), phase(quarter, child)]
    return np.stack([signed * side[None, None, :] for side in sides])


def stage_complex(first, count):
    out = np.eye(R, dtype=np.complex128).reshape(1, R, 1, R)
    for level in range(first, first + count):
        step = level_matrix(level)
        joined = np.einsum("etju,aubs->aetjbs", step, out)
        n = out.shape[0]
        out = joined.reshape(2 * n, R, 2 * n, R)
    return out


def real_form(mat):
    n, m = mat.shape[0], mat.shape[2]
    out = np.zeros((n, 2, R, m, 2, R))
    out[:, 0, :, :, 0] = mat.real
    out[:, 0, :, :, 1] = -mat.imag
    out[:, 1, :, :, 0] = mat.imag
    out[:, 1, :, :, 1] = mat.real
    return out.reshape(n * 2 * R, m * 2 * R)


def leaf_map():
    nodes = node_offsets(CELLS)
    angles = np.pi * (np.arange(R) + 0.5) / R
    at_exact = lagrange_values(2.0 * nodes / CELLS - 1.0, np.cos(angles))
    cheb = np.stack([np.cos(n * angles) for n in range(R)])
    norm = np.where(np.arange(R) == 0, 1.0, 2.0) / R
    coef = (norm[:, None] * (cheb @ at_exact.T)).astype(np.float32).astype(np.float64)
    split = np.zeros((R, R))
    for n in range(8):
        split[n, n] = 1.0
    split[8, 8] = 1.0
    for i in range(1, 8):
        split[8 + i, 8 + i] = 2.0
        split[8 + i, 8 - i] -= 1.0
    return coef.T @ split


def stage_tables():
    mats = []
    leaf = leaf_map()
    first = stage_complex(0, 3)
    mats.append(real_form(np.einsum("atbs,sn->atbn", first, leaf)))
    mats.append(real_form(stage_complex(3, 3)))
    mats.append(real_form(stage_complex(6, 3)))
    two = stage_complex(9, 2)
    wide = np.einsum("atbs,ij->aitbjs", two, np.eye(2)).reshape(8, R, 8, R)
    mats.append(real_form(wide))
    mats.append(real_form(stage_complex(11, 3)))
    mats.append(real_form(stage_complex(14, 3)))
    return np.stack(mats)


def top_frequency():
    nodes = node_offsets(CELLS << 17)
    q = np.arange(N_BLK)[:, None]
    return nodes, nodes[None, :] / 2.0**32 + q / 256.0


def hi_lo(table):
    full = np.asarray(table, np.float32)
    hi = full.astype(jnp.bfloat16)
    lo = (full - hi.astype(np.float32)).astype(jnp.bfloat16)
    return hi, lo


@functools.lru_cache(None)
def tables():
    hi, lo = hi_lo(stage_tables())
    stages = np.stack([hi, lo], axis=1)
    nodes, freq = top_frequency()
    y = np.arange(HALF) + 0.5
    angle = 2.0 * np.pi * ((freq.reshape(-1)[:, None] * y[None, :]) % 1.0)
    wave_hi, wave_lo = hi_lo(np.concatenate([np.cos(angle), np.sin(angle)], axis=1))
    waves = np.concatenate([wave_hi, wave_hi, wave_lo, wave_lo], axis=0)
    q = np.arange(N_BLK)[:, None]
    shift = np.exp(2j * np.pi * ((-0.5 * nodes[None, :] / 2.0**32 + q * (HALF - 0.5) / 256.0) % 1.0))
    shift = np.concatenate([shift.real, shift.imag], axis=1).astype(np.float32)
    shift = np.broadcast_to(shift[:, :, None], (N_BLK, 2 * R, 128)).copy()
    turns = (3 * np.arange(CELLS)) % CELLS / CELLS
    spin = np.stack([np.cos(2 * np.pi * turns), np.sin(2 * np.pi * turns)]).astype(np.float32)
    spin = np.broadcast_to(spin[:, None, :], (2, 8, CELLS)).copy()
    return stages, waves, shift, spin


def swap_lane(blocks, row_bit, lane_bit):
    out = list(blocks)
    amount = 1 << lane_bit
    for i in range(len(blocks)):
        if i >> row_bit & 1:
            continue
        k = i | 1 << row_bit
        x0, x1 = blocks[i], blocks[k]
        mask = (lax.broadcasted_iota(jnp.int32, x0.shape, 1) & amount) != 0
        out[i] = jnp.where(mask, pltpu.roll(x1, amount, 1), x0)
        out[k] = jnp.where(mask, x1, pltpu.roll(x0, 128 - amount, 1))
    return out


def swap_half(left, right, row_bit):
    left, right = list(left), list(right)
    for i in range(len(left)):
        if i >> row_bit & 1:
            continue
        k = i | 1 << row_bit
        left[k], right[i] = right[i], left[k]
    return left, right


def gather_rows(blocks):
    return jnp.concatenate(blocks, axis=0)


def split_rows(x, rows):
    return [x[i * rows : (i + 1) * rows] for i in range(x.shape[0] // rows)]


def apply_stage(stage_ref, index, left, right):
    x = jnp.concatenate([left, right], axis=1)
    hi = x.astype(jnp.bfloat16)
    lo = (x - hi.astype(jnp.float32)).astype(jnp.bfloat16)
    w_hi, w_lo = stage_ref[index, 0], stage_ref[index, 1]
    dot = functools.partial(jnp.dot, preferred_element_type=jnp.float32)
    y = dot(w_hi, hi) + (dot(w_lo, hi) + dot(w_hi, lo))
    return y[:, :128], y[:, 128:]


LAG = 4


def leaf_sums(pos, amp, spin_re, spin_im, mom, half):
    def beta_step(beta, carry):
        cells, amp_re, amp_im = [], [], []
        for group in range(16):
            s7, s6, s10, s9 = group >> 3 & 1, group >> 2 & 1, group >> 1 & 1, group & 1
            slab, rows = s10 * 2 + s9, pl.ds(beta + s6 * 64 + s7 * 128, 8, stride=8)
            cell = pos[slab, half, rows, :] & (CELLS - 1)
            sr, si = amp[0, slab, half, rows, :], amp[1, slab, half, rows, :]
            wr = jnp.take_along_axis(spin_re, cell, axis=1)
            wi = jnp.take_along_axis(spin_im, cell, axis=1)
            cells.append(cell.astype(jnp.float32) * (2.0 / CELLS) - 1.0)
            amp_re.append(wr * sr - wi * si)
            amp_im.append(wi * sr + wr * si)
        v_all = jnp.concatenate(cells, axis=0).T
        re_all = jnp.concatenate(amp_re, axis=0).T
        im_all = jnp.concatenate(amp_im, axis=0).T
        acc = [None] * 32
        for step in range(16):
            rows = slice(step * 8, step * 8 + 8)
            v, sr, si = v_all[rows], re_all[rows], im_all[rows]
            cheb = [None, v]
            twice = v + v
            cheb.append(twice * v - 1.0)
            for n in range(3, 9):
                cheb.append(twice * cheb[-1] - cheb[-2])
            for side, (a, b) in enumerate(((sr, si), (cheb[8] * sr, cheb[8] * si))):
                for n in range(8):
                    pa = a if n == 0 else cheb[n] * a
                    pb = b if n == 0 else cheb[n] * b
                    ia, ib = side * 8 + n, 16 + side * 8 + n
                    acc[ia] = pa if acc[ia] is None else acc[ia] + pa
                    acc[ib] = pb if acc[ib] is None else acc[ib] + pb
        for n in range(32):
            mom[beta, n : n + 1, half * 128 : half * 128 + 128] = jnp.sum(acc[n], axis=0, keepdims=True)
        return carry

    lax.fori_loop(0, 8, beta_step, 0)


def lane_swaps(x, pairs):
    blocks = split_rows(x, 32)
    for row_bit, lane_bit in pairs:
        blocks = swap_lane(blocks, row_bit, lane_bit)
    return blocks


def local_tree(stage, mom, out):
    sums = mom[...].reshape(256, 256)
    left, right = apply_stage(stage, 0, sums[:, :128], sums[:, 128:])
    pairs = ((2, 2), (1, 1), (0, 0))
    left, right = apply_stage(
        stage, 1, gather_rows(lane_swaps(left, pairs)), gather_rows(lane_swaps(right, pairs))
    )
    pairs = ((1, 6), (0, 5))
    left, right = swap_half(lane_swaps(left, pairs), lane_swaps(right, pairs), 2)
    left, right = apply_stage(stage, 2, gather_rows(left), gather_rows(right))
    pairs = ((2, 4), (1, 3), (0, 2))
    left, right = apply_stage(
        stage, 3, gather_rows(lane_swaps(left, pairs)), gather_rows(lane_swaps(right, pairs))
    )
    for half, x in enumerate((left, right)):
        tiles = split_rows(x, 8)
        tiles = swap_lane(swap_lane(tiles, 1, 1), 0, 0)
        for i in range(32):
            e9, e10, e0, e1, e2 = i >> 4 & 1, i >> 3 & 1, i >> 2 & 1, i >> 1 & 1, i & 1
            out[e0 * 32 + e1 * 16 + e2 * 8 + e9 * 4 + e10 * 2 + half] = tiles[i]


def cross_tree(stage, shift, got, out):
    halves = []
    for half in range(2):
        tiles = [None] * 32
        for d in range(32):
            tiles[(d & 7) * 4 + (d >> 4 & 1) * 2 + (d >> 3 & 1)] = got[half * 32 + d]
        halves.append(swap_lane(swap_lane(tiles, 1, 1), 0, 0))
    left, right = apply_stage(stage, 4, gather_rows(halves[0]), gather_rows(halves[1]))
    pairs = ((1, 1), (0, 0))
    left, right = swap_half(lane_swaps(left, pairs), lane_swaps(right, pairs), 2)
    left, right = apply_stage(stage, 5, gather_rows(left), gather_rows(right))
    shift_re, shift_im = shift[:R], shift[R:]
    for half, x in enumerate((left, right)):
        turned = []
        for block in split_rows(x, 32):
            re, im = block[:R], block[R:]
            turned.append(shift_re * re - shift_im * im)
            turned.append(shift_im * re + shift_re * im)
        tiles = split_rows(gather_rows(turned), 8)
        tiles = swap_lane(swap_lane(tiles, 1, 1), 0, 0)
        for i in range(32):
            e14, e15, e16, e12, e13 = i >> 4 & 1, i >> 3 & 1, i >> 2 & 1, i >> 1 & 1, i & 1
            out[half + e12 * 2 + e13 * 4 + e14 * 8 + e15 * 16 + e16 * 32] = tiles[i]


def coefficients(roots, z):
    parts = [[], []]
    for q in range(N_BLK):
        for half in range(2):
            tiles = [roots[q, z * 8 + (c * 2 + half)] for c in range(4)]
            parts[half].append(swap_lane(swap_lane(tiles, 1, 1), 0, 0))
    lhs, inverse = [[], []], []
    for half in range(2):
        sides = []
        for c in range(2):
            rows = []
            for q in range(N_BLK):
                rows += parts[half][q][2 * c : 2 * c + 2]
            sides.append(jnp.concatenate(rows, axis=0))
        reach = [jnp.sum(jnp.abs(x), axis=0, keepdims=True) for x in sides]
        reach = jnp.maximum(jnp.maximum(reach[0], reach[1]), 1e-30)
        scale = SPAN / reach
        inverse.append(jnp.broadcast_to(reach * (1.0 / SPAN), (8, 128)))
        for c, x in enumerate(sides):
            x = x * scale
            hi = x.astype(jnp.bfloat16).astype(jnp.float32)
            t = jnp.concatenate([hi, x - hi], axis=0).T.astype(jnp.bfloat16)
            lhs[c].append(jnp.concatenate([t, t], axis=1))
    inverse = jnp.concatenate([jnp.concatenate(inverse, axis=1), jnp.zeros((120, 256), jnp.float32)], axis=0)
    columns = jnp.concatenate([inverse[:, :128].T, inverse[:, 128:].T], axis=0)
    return jnp.concatenate(lhs[0] + lhs[1], axis=0), columns


def fill_dense(lhs, wave, dense):
    for n in range(6):
        cols = slice(n * 256, n * 256 + 256)
        sums = jnp.dot(lhs, wave[:, cols], preferred_element_type=jnp.float32)
        sums = (sums + (32768.0 + 0.5)).astype(jnp.int32)
        dense[:, cols] = (sums[:256] << 16) | sums[256:]


def look_up(dense, columns, tick, out, z, reverse):
    sub = lax.broadcasted_iota(jnp.int32, (8, 128), 0)
    for i in range(32):
        row = i * 8
        base = z * 256 + row
        y = tick[pl.ds(base, 8), :] - ((base + sub) * 64 + reverse) * BOX_TICKS - HALF
        upper = y >= 0
        index = jnp.where(upper, y, -1 - y)
        low, high = index & 127, index >> 7
        pairs = [None, None]
        for h in range(6):
            pick = high == h
            for part in range(2):
                start = part * HALF + h * 128
                got = jnp.take_along_axis(dense[row : row + 8, start : start + 128], low, axis=1)
                pairs[part] = got if h == 0 else jnp.where(pick, got, pairs[part])
        even, odd = pairs
        re_even, im_even = lax.shift_right_logical(even, 16) - 32768, (even & 65535) - 32768
        re_odd, im_odd = lax.shift_right_logical(odd, 16) - 32768, (odd & 65535) - 32768
        unit = jnp.broadcast_to(columns[row : row + 8, 0:1], (8, 128))
        re = jnp.where(upper, re_even - im_odd, re_even + im_odd)
        im = jnp.where(upper, im_even + re_odd, im_even - re_odd)
        out[pl.ds(base * 2, 8, stride=2), :] = re.astype(jnp.float32) * unit
        out[pl.ds(base * 2 + 1, 8, stride=2), :] = im.astype(jnp.float32) * unit


def kernel(
    pos_in, amp_in, tick_in, stage_in, wave_in, shift_in, spin_in, out_hbm,
    pos, amp, tick, stage, wave, shift, spin, mom,
    first_src, first_dst, second_src, roots, out, dense,
    load_sem, store_sem, send1, recv1, send2, recv2, send3, recv3,
):
    leaf, blk = lax.axis_index("leaf"), lax.axis_index("blk")
    own_z = leaf // 8

    loads = [
        pltpu.make_async_copy(spin_in, spin, load_sem.at[0]),
        pltpu.make_async_copy(pos_in.at[:, 0], pos.at[:, 0], load_sem.at[1]),
        pltpu.make_async_copy(amp_in.at[:, :, 0], amp.at[:, :, 0], load_sem.at[2]),
        pltpu.make_async_copy(pos_in.at[:, 1], pos.at[:, 1], load_sem.at[3]),
        pltpu.make_async_copy(amp_in.at[:, :, 1], amp.at[:, :, 1], load_sem.at[4]),
        pltpu.make_async_copy(stage_in, stage, load_sem.at[5]),
        pltpu.make_async_copy(shift_in.at[blk], shift, load_sem.at[6]),
        pltpu.make_async_copy(wave_in, wave, load_sem.at[7]),
        pltpu.make_async_copy(tick_in, tick, load_sem.at[8]),
    ]
    for load in loads[:3]:
        load.start()
    barrier = pltpu.get_barrier_semaphore()

    def greet(i, carry):
        pl.semaphore_signal(barrier, inc=1, device_id={"leaf": leaf ^ i}, device_id_type=MESH)
        return carry

    lax.fori_loop(1, 64, greet, 0)
    for i in range(1, N_BLK):
        pl.semaphore_signal(barrier, inc=1, device_id={"blk": (blk + i) % N_BLK}, device_id_type=MESH)

    for load in loads[3:5]:
        load.start()
    for load in loads[:3]:
        load.wait()
    for load in loads[5:]:
        load.start()
    spin_re, spin_im = spin[0], spin[1]
    leaf_sums(pos, amp, spin_re, spin_im, mom, 0)
    for load in loads[3:5]:
        load.wait()
    leaf_sums(pos, amp, spin_re, spin_im, mom, 1)
    loads[5].wait()
    local_tree(stage, mom, first_src)
    pl.semaphore_wait(barrier, 63 + N_BLK - 1)

    def first(i):
        return pltpu.make_async_remote_copy(
            src_ref=first_src.at[leaf ^ i],
            dst_ref=first_dst.at[leaf],
            send_sem=send1.at[i],
            recv_sem=recv1.at[i],
            device_id={"leaf": leaf ^ i},
            device_id_type=MESH,
        )

    def far_first(n):
        k = n // 8
        step = (k + 1) // 2
        off = (4 + step * (1 - 2 * (k % 2)) + 8) % 8
        z = (own_z + off) % 8
        return (z * 8 + n % 8) ^ leaf

    def first_send(n, carry):
        i = far_first(n)

        @pl.when(i != 0)
        def _():
            first(i).start()

        return carry

    def first_wait(i, carry):
        first(i).wait()
        return carry

    lax.fori_loop(0, 64, first_send, 0)
    first_dst[leaf] = first_src[leaf]
    loads[6].wait()
    lax.fori_loop(1, 64, first_wait, 0)
    cross_tree(stage, shift[...], first_dst, second_src)

    def near_z(c):
        k = (c + 1) // 2
        return (own_z + k * (2 * (c % 2) - 1) + 8) % 8

    def second(c, j):
        other = near_z(c) * 8 + j
        return pltpu.make_async_remote_copy(
            src_ref=second_src.at[other],
            dst_ref=roots.at[blk, leaf],
            send_sem=send2.at[other],
            recv_sem=recv2.at[leaf],
            device_id={"leaf": other},
            device_id_type=MESH,
        )

    def second_got(z, j):
        other = z * 8 + j
        return pltpu.make_async_remote_copy(
            src_ref=second_src.at[other],
            dst_ref=roots.at[blk, other],
            send_sem=send2.at[other],
            recv_sem=recv2.at[other],
            device_id={"leaf": other},
            device_id_type=MESH,
        )

    own_j = leaf % 8

    def send_own(i, carry):
        second(0, (own_j + i) % 8).start()
        return carry

    lax.fori_loop(1, 8, send_own, 0)

    def send_far(n, carry):
        second(n // 8, (own_j + n) % 8).start()
        return carry

    lax.fori_loop(8, 64, send_far, 0)
    roots[blk, leaf] = second_src[leaf]
    loads[7].wait()
    loads[8].wait()

    def third(z, i):
        return pltpu.make_async_remote_copy(
            src_ref=roots.at[blk, pl.ds(z * 8, 8)],
            dst_ref=roots.at[blk, pl.ds(z * 8, 8)],
            send_sem=send3.at[z, i],
            recv_sem=recv3.at[z, i],
            device_id={"blk": (blk + i) % N_BLK},
            device_id_type=MESH,
        )

    def third_got(z, i):
        source = (blk + N_BLK - i) % N_BLK
        return pltpu.make_async_remote_copy(
            src_ref=roots.at[blk, pl.ds(z * 8, 8)],
            dst_ref=roots.at[source, pl.ds(z * 8, 8)],
            send_sem=send3.at[z, i],
            recv_sem=recv3.at[z, i],
            device_id={"blk": (blk + i) % N_BLK},
            device_id_type=MESH,
        )

    def store(z):
        return pltpu.make_async_copy(
            out.at[pl.ds(z * 512, 512)], out_hbm.at[pl.ds(z * 512, 512)], store_sem.at[z]
        )

    reverse = jnp.int32(0)
    for bit in range(6):
        reverse = reverse * 2 + (leaf // 2**bit) % 2

    def chunk_step(c, carry):
        @pl.when(c < 8)
        def _():
            z = near_z(c)

            def got(j, carry):
                second_got(z, (own_j + j) % 8).wait_recv()
                return carry

            lax.fori_loop(jnp.where(c == 0, 1, 0), 8, got, 0)
            for i in (2, 1, 3):
                third(z, i).start()

        @pl.when(c >= LAG)
        def _():
            z = near_z(c - LAG)
            for i in (1, 2, 3):
                third_got(z, i).wait_recv()
            lhs, columns = coefficients(roots, z)
            fill_dense(lhs, wave, dense)
            look_up(dense, columns, tick, out, z, reverse)
            store(z).start()

        return carry

    lax.fori_loop(0, 8 + LAG, chunk_step, 0)

    def finish(z, carry):
        store(z).wait()
        for i in (1, 2, 3):
            third(z, i).wait_send()
        return carry

    lax.fori_loop(0, 8, finish, 0)

    def finish_second(i, carry):
        second_got(0, leaf ^ i).wait_send()
        return carry

    lax.fori_loop(1, 64, finish_second, 0)


def local(src_pos, strengths, tgt_pos):
    stages, waves, shift, spin = tables()
    hbm = pl.BlockSpec(memory_space=pl.ANY)
    vmem, dma = pltpu.VMEM, pltpu.SemaphoreType.DMA
    f32, tiles = jnp.float32, (64, 8, 128)
    out = pl.pallas_call(
        kernel,
        out_shape=jax.ShapeDtypeStruct((4096, 128), f32),
        in_specs=[hbm] * 7,
        out_specs=hbm,
        scratch_shapes=[
            vmem((4, 2, 256, 128), jnp.int32),
            vmem((2, 4, 2, 256, 128), f32),
            vmem((2048, 128), jnp.int32),
            vmem((6, 2, 256, 256), jnp.bfloat16),
            vmem((256, 2 * HALF), jnp.bfloat16),
            vmem((2 * R, 128), f32),
            vmem((2, 8, 128), f32),
            vmem((8, 32, 256), f32),
            vmem(tiles, f32),
            vmem(tiles, f32),
            vmem(tiles, f32),
            vmem((N_BLK, *tiles), f32),
            vmem((4096, 128), f32),
            vmem((256, 2 * HALF), jnp.int32),
            dma((9,)),
            dma((8,)),
            dma((64,)),
            dma((64,)),
            dma((64,)),
            dma((64,)),
            dma((8, N_BLK)),
            dma((8, N_BLK)),
        ],
        compiler_params=pltpu.CompilerParams(collective_id=0, has_side_effects=True),
        name="butterfly",
    )(
        src_pos.reshape(4, 2, 256, 128),
        strengths.reshape(2, 4, 2, 256, 128),
        tgt_pos.reshape(2048, 128),
        jnp.asarray(stages),
        jnp.asarray(waves),
        jnp.asarray(shift),
        jnp.asarray(spin),
    )
    return jnp.transpose(out.reshape(2048, 2, 128), (1, 0, 2)).reshape(2, 2048 * 128)


def solution(mesh):
    return jax.shard_map(
        local,
        mesh=mesh,
        in_specs=(P("blk", "leaf"), P(None, "blk", "leaf"), P(("leaf", "blk"))),
        out_specs=P(None, ("leaf", "blk")),
        check_vma=False,
    )
```

```python
import functools
import math

import jax
import jax.numpy as jnp
import numpy as np
from jax import lax
from jax.experimental import pallas as pl
from jax.experimental.pallas import tpu as pltpu
from jax.sharding import PartitionSpec as P

R = 16
CELLS = 128
TOP_TICKS = 201326592
BOX_TICKS = 1536
HALF = BOX_TICKS // 2
N_BLK = 4
MESH = pl.DeviceIdType.MESH
SPAN = 32000.0


def node_offsets(box_cells):
    unit = (1.0 - np.cos(np.pi * (np.arange(R) + 0.5) / R)) / 2.0
    return np.floor(box_cells * unit).astype(np.int64)


def lagrange_values(node_pos, points):
    rows = []
    for a in range(node_pos.shape[0]):
        col = np.ones(points.shape[0])
        for b in range(node_pos.shape[0]):
            if b != a:
                col = col * (points - node_pos[b]) / (node_pos[a] - node_pos[b])
        rows.append(col)
    return np.stack(rows)


def phase(ticks, cells):
    product = (int(ticks) * np.asarray(cells, np.int64)) % (1 << 32)
    return np.exp(2j * np.pi * product / 2.0**32)


def level_matrix(level):
    cells = CELLS << level
    child, parent = node_offsets(cells), node_offsets(2 * cells)
    inner = np.concatenate([child, child + cells])
    blend = lagrange_values(parent / (2.0 * cells), inner / (2.0 * cells))
    blend = blend.astype(np.float32).astype(np.float64).reshape(R, 2, R)
    signed = blend * np.array([1.0, -1.0])[None, :, None]
    quarter = (TOP_TICKS >> level) // 4
    sides = [phase(-quarter, child), phase(quarter, child)]
    return np.stack([signed * side[None, None, :] for side in sides])


def stage_complex(first, count):
    out = np.eye(R, dtype=np.complex128).reshape(1, R, 1, R)
    for level in range(first, first + count):
        step = level_matrix(level)
        joined = np.einsum("etju,aubs->aetjbs", step, out)
        n = out.shape[0]
        out = joined.reshape(2 * n, R, 2 * n, R)
    return out


def real_form(mat):
    n, m = mat.shape[0], mat.shape[2]
    out = np.zeros((n, 2, R, m, 2, R))
    out[:, 0, :, :, 0] = mat.real
    out[:, 0, :, :, 1] = -mat.imag
    out[:, 1, :, :, 0] = mat.imag
    out[:, 1, :, :, 1] = mat.real
    return out.reshape(n * 2 * R, m * 2 * R)


def leaf_map():
    nodes = node_offsets(CELLS)
    angles = np.pi * (np.arange(R) + 0.5) / R
    at_exact = lagrange_values(2.0 * nodes / CELLS - 1.0, np.cos(angles))
    cheb = np.stack([np.cos(n * angles) for n in range(R)])
    norm = np.where(np.arange(R) == 0, 1.0, 2.0) / R
    coef = (norm[:, None] * (cheb @ at_exact.T)).astype(np.float32).astype(np.float64)
    split = np.zeros((R, R))
    for n in range(8):
        split[n, n] = 1.0
    split[8, 8] = 1.0
    for i in range(1, 8):
        split[8 + i, 8 + i] = 2.0
        split[8 + i, 8 - i] -= 1.0
    return coef.T @ split


def stage_tables():
    mats = []
    leaf = leaf_map()
    first = stage_complex(0, 3)
    mats.append(real_form(np.einsum("atbs,sn->atbn", first, leaf)))
    mats.append(real_form(stage_complex(3, 3)))
    mats.append(real_form(stage_complex(6, 3)))
    two = stage_complex(9, 2)
    wide = np.einsum("atbs,ij->aitbjs", two, np.eye(2)).reshape(8, R, 8, R)
    mats.append(real_form(wide))
    mats.append(real_form(stage_complex(11, 3)))
    mats.append(real_form(stage_complex(14, 3)))
    return np.stack(mats)


def top_frequency():
    nodes = node_offsets(CELLS << 17)
    q = np.arange(N_BLK)[:, None]
    return nodes, nodes[None, :] / 2.0**32 + q / 256.0


def hi_lo(table):
    full = np.asarray(table, np.float32)
    hi = full.astype(jnp.bfloat16)
    lo = (full - hi.astype(np.float32)).astype(jnp.bfloat16)
    return hi, lo


@functools.lru_cache(None)
def tables():
    hi, lo = hi_lo(stage_tables())
    stages = np.stack([hi, lo], axis=1)
    nodes, freq = top_frequency()
    y = np.arange(HALF) + 0.5
    angle = 2.0 * np.pi * ((freq.reshape(-1)[:, None] * y[None, :]) % 1.0)
    wave_hi, wave_lo = hi_lo(np.concatenate([np.cos(angle), np.sin(angle)], axis=1))
    waves = np.concatenate([wave_hi, wave_hi, wave_lo, wave_lo], axis=0)
    q = np.arange(N_BLK)[:, None]
    shift = np.exp(2j * np.pi * ((-0.5 * nodes[None, :] / 2.0**32 + q * (HALF - 0.5) / 256.0) % 1.0))
    shift = np.concatenate([shift.real, shift.imag], axis=1).astype(np.float32)
    shift = np.broadcast_to(shift[:, :, None], (N_BLK, 2 * R, 128)).copy()
    turns = (3 * np.arange(CELLS)) % CELLS / CELLS
    spin = np.stack([np.cos(2 * np.pi * turns), np.sin(2 * np.pi * turns)]).astype(np.float32)
    spin = np.broadcast_to(spin[:, None, :], (2, 8, CELLS)).copy()
    return stages, waves, shift, spin


def swap_lane(blocks, row_bit, lane_bit):
    out = list(blocks)
    amount = 1 << lane_bit
    for i in range(len(blocks)):
        if i >> row_bit & 1:
            continue
        k = i | 1 << row_bit
        x0, x1 = blocks[i], blocks[k]
        mask = (lax.broadcasted_iota(jnp.int32, x0.shape, 1) & amount) != 0
        out[i] = jnp.where(mask, pltpu.roll(x1, amount, 1), x0)
        out[k] = jnp.where(mask, x1, pltpu.roll(x0, 128 - amount, 1))
    return out


def swap_half(left, right, row_bit):
    left, right = list(left), list(right)
    for i in range(len(left)):
        if i >> row_bit & 1:
            continue
        k = i | 1 << row_bit
        left[k], right[i] = right[i], left[k]
    return left, right


def gather_rows(blocks):
    return jnp.concatenate(blocks, axis=0)


def split_rows(x, rows):
    return [x[i * rows : (i + 1) * rows] for i in range(x.shape[0] // rows)]


def apply_stage(stage_ref, index, left, right):
    x = jnp.concatenate([left, right], axis=1)
    hi = x.astype(jnp.bfloat16)
    lo = (x - hi.astype(jnp.float32)).astype(jnp.bfloat16)
    w_hi, w_lo = stage_ref[index, 0], stage_ref[index, 1]
    dot = functools.partial(jnp.dot, preferred_element_type=jnp.float32)
    y = dot(w_hi, hi) + (dot(w_lo, hi) + dot(w_hi, lo))
    return y[:, :128], y[:, 128:]


LAG = 4


def leaf_sums(pos, amp, spin_re, spin_im, mom, half):
    def beta_step(beta, carry):
        cells, amp_re, amp_im = [], [], []
        for group in range(16):
            s7, s6, s10, s9 = group >> 3 & 1, group >> 2 & 1, group >> 1 & 1, group & 1
            slab, rows = s10 * 2 + s9, pl.ds(beta + s6 * 64 + s7 * 128, 8, stride=8)
            cell = pos[slab, half, rows, :] & (CELLS - 1)
            sr, si = amp[0, slab, half, rows, :], amp[1, slab, half, rows, :]
            wr = jnp.take_along_axis(spin_re, cell, axis=1)
            wi = jnp.take_along_axis(spin_im, cell, axis=1)
            cells.append(cell.astype(jnp.float32) * (2.0 / CELLS) - 1.0)
            amp_re.append(wr * sr - wi * si)
            amp_im.append(wi * sr + wr * si)
        v_all = jnp.concatenate(cells, axis=0).T
        re_all = jnp.concatenate(amp_re, axis=0).T
        im_all = jnp.concatenate(amp_im, axis=0).T
        acc = [None] * 32
        for step in range(16):
            rows = slice(step * 8, step * 8 + 8)
            v, sr, si = v_all[rows], re_all[rows], im_all[rows]
            cheb = [None, v]
            twice = v + v
            cheb.append(twice * v - 1.0)
            for n in range(3, 9):
                cheb.append(twice * cheb[-1] - cheb[-2])
            for side, (a, b) in enumerate(((sr, si), (cheb[8] * sr, cheb[8] * si))):
                for n in range(8):
                    pa = a if n == 0 else cheb[n] * a
                    pb = b if n == 0 else cheb[n] * b
                    ia, ib = side * 8 + n, 16 + side * 8 + n
                    acc[ia] = pa if acc[ia] is None else acc[ia] + pa
                    acc[ib] = pb if acc[ib] is None else acc[ib] + pb
        for n in range(32):
            mom[beta, n : n + 1, half * 128 : half * 128 + 128] = jnp.sum(acc[n], axis=0, keepdims=True)
        return carry

    lax.fori_loop(0, 8, beta_step, 0)


def lane_swaps(x, pairs):
    blocks = split_rows(x, 32)
    for row_bit, lane_bit in pairs:
        blocks = swap_lane(blocks, row_bit, lane_bit)
    return blocks


def local_tree(stage, mom, out):
    sums = mom[...].reshape(256, 256)
    left, right = apply_stage(stage, 0, sums[:, :128], sums[:, 128:])
    pairs = ((2, 2), (1, 1), (0, 0))
    left, right = apply_stage(
        stage, 1, gather_rows(lane_swaps(left, pairs)), gather_rows(lane_swaps(right, pairs))
    )
    pairs = ((1, 6), (0, 5))
    left, right = swap_half(lane_swaps(left, pairs), lane_swaps(right, pairs), 2)
    left, right = apply_stage(stage, 2, gather_rows(left), gather_rows(right))
    pairs = ((2, 4), (1, 3), (0, 2))
    left, right = apply_stage(
        stage, 3, gather_rows(lane_swaps(left, pairs)), gather_rows(lane_swaps(right, pairs))
    )
    for half, x in enumerate((left, right)):
        tiles = split_rows(x, 8)
        tiles = swap_lane(swap_lane(tiles, 1, 1), 0, 0)
        for i in range(32):
            e9, e10, e0, e1, e2 = i >> 4 & 1, i >> 3 & 1, i >> 2 & 1, i >> 1 & 1, i & 1
            out[e0 * 32 + e1 * 16 + e2 * 8 + e9 * 4 + e10 * 2 + half] = tiles[i]


def cross_tree(stage, shift, got, out):
    halves = []
    for half in range(2):
        tiles = [None] * 32
        for d in range(32):
            tiles[(d & 7) * 4 + (d >> 4 & 1) * 2 + (d >> 3 & 1)] = got[half * 32 + d]
        halves.append(swap_lane(swap_lane(tiles, 1, 1), 0, 0))
    left, right = apply_stage(stage, 4, gather_rows(halves[0]), gather_rows(halves[1]))
    pairs = ((1, 1), (0, 0))
    left, right = swap_half(lane_swaps(left, pairs), lane_swaps(right, pairs), 2)
    left, right = apply_stage(stage, 5, gather_rows(left), gather_rows(right))
    shift_re, shift_im = shift[:R], shift[R:]
    for half, x in enumerate((left, right)):
        turned = []
        for block in split_rows(x, 32):
            re, im = block[:R], block[R:]
            turned.append(shift_re * re - shift_im * im)
            turned.append(shift_im * re + shift_re * im)
        tiles = split_rows(gather_rows(turned), 8)
        tiles = swap_lane(swap_lane(tiles, 1, 1), 0, 0)
        for i in range(32):
            e14, e15, e16, e12, e13 = i >> 4 & 1, i >> 3 & 1, i >> 2 & 1, i >> 1 & 1, i & 1
            out[half + e12 * 2 + e13 * 4 + e14 * 8 + e15 * 16 + e16 * 32] = tiles[i]


def coefficients(roots, z):
    parts = [[], []]
    for q in range(N_BLK):
        for half in range(2):
            tiles = [roots[q, z * 8 + (c * 2 + half)] for c in range(4)]
            parts[half].append(swap_lane(swap_lane(tiles, 1, 1), 0, 0))
    lhs, inverse = [[], []], []
    for half in range(2):
        sides = []
        for c in range(2):
            rows = []
            for q in range(N_BLK):
                rows += parts[half][q][2 * c : 2 * c + 2]
            sides.append(jnp.concatenate(rows, axis=0))
        reach = [jnp.sum(jnp.abs(x), axis=0, keepdims=True) for x in sides]
        reach = jnp.maximum(jnp.maximum(reach[0], reach[1]), 1e-30)
        scale = SPAN / reach
        inverse.append(jnp.broadcast_to(reach * (1.0 / SPAN), (8, 128)))
        for c, x in enumerate(sides):
            x = x * scale
            hi = x.astype(jnp.bfloat16).astype(jnp.float32)
            t = jnp.concatenate([hi, x - hi], axis=0).T.astype(jnp.bfloat16)
            lhs[c].append(jnp.concatenate([t, t], axis=1))
    inverse = jnp.concatenate([jnp.concatenate(inverse, axis=1), jnp.zeros((120, 256), jnp.float32)], axis=0)
    columns = jnp.concatenate([inverse[:, :128].T, inverse[:, 128:].T], axis=0)
    return jnp.concatenate(lhs[0] + lhs[1], axis=0), columns


def fill_dense(lhs, wave, dense):
    for n in range(6):
        cols = slice(n * 256, n * 256 + 256)
        sums = jnp.dot(lhs, wave[:, cols], preferred_element_type=jnp.float32)
        sums = (sums + (32768.0 + 0.5)).astype(jnp.int32)
        dense[:, cols] = (sums[:256] << 16) | sums[256:]


def look_up(dense, columns, tick, out, z, reverse):
    sub = lax.broadcasted_iota(jnp.int32, (8, 128), 0)
    for i in range(32):
        row = i * 8
        base = z * 256 + row
        y = tick[pl.ds(base, 8), :] - ((base + sub) * 64 + reverse) * BOX_TICKS - HALF
        upper = y >= 0
        index = jnp.where(upper, y, -1 - y)
        low, high = index & 127, index >> 7
        pairs = [None, None]
        for h in range(6):
            pick = high == h
            for part in range(2):
                start = part * HALF + h * 128
                got = jnp.take_along_axis(dense[row : row + 8, start : start + 128], low, axis=1)
                pairs[part] = got if h == 0 else jnp.where(pick, got, pairs[part])
        even, odd = pairs
        re_even, im_even = lax.shift_right_logical(even, 16) - 32768, (even & 65535) - 32768
        re_odd, im_odd = lax.shift_right_logical(odd, 16) - 32768, (odd & 65535) - 32768
        unit = jnp.broadcast_to(columns[row : row + 8, 0:1], (8, 128))
        re = jnp.where(upper, re_even - im_odd, re_even + im_odd)
        im = jnp.where(upper, im_even + re_odd, im_even - re_odd)
        out[pl.ds(base * 2, 8, stride=2), :] = re.astype(jnp.float32) * unit
        out[pl.ds(base * 2 + 1, 8, stride=2), :] = im.astype(jnp.float32) * unit


def kernel(
    pos_in, amp_in, tick_in, stage_in, wave_in, shift_in, spin_in, out,
    pos, amp, tick, stage, wave, shift, spin, mom,
    first_src, first_dst, second_src, roots, dense,
    load_sem, send1, recv1, send2, recv2, send3, recv3,
):
    leaf, blk = lax.axis_index("leaf"), lax.axis_index("blk")
    own_z = leaf // 8

    loads = [
        pltpu.make_async_copy(spin_in, spin, load_sem.at[0]),
        pltpu.make_async_copy(pos_in.at[:, 0], pos.at[:, 0], load_sem.at[1]),
        pltpu.make_async_copy(amp_in.at[:, :, 0], amp.at[:, :, 0], load_sem.at[2]),
        pltpu.make_async_copy(pos_in.at[:, 1], pos.at[:, 1], load_sem.at[3]),
        pltpu.make_async_copy(amp_in.at[:, :, 1], amp.at[:, :, 1], load_sem.at[4]),
        pltpu.make_async_copy(stage_in, stage, load_sem.at[5]),
        pltpu.make_async_copy(shift_in.at[blk], shift, load_sem.at[6]),
        pltpu.make_async_copy(wave_in, wave, load_sem.at[7]),
        pltpu.make_async_copy(tick_in, tick, load_sem.at[8]),
    ]
    for load in loads[:3]:
        load.start()
    barrier = pltpu.get_barrier_semaphore()

    def greet(i, carry):
        pl.semaphore_signal(barrier, inc=1, device_id={"leaf": leaf ^ i}, device_id_type=MESH)
        return carry

    lax.fori_loop(1, 64, greet, 0)
    for i in range(1, N_BLK):
        pl.semaphore_signal(barrier, inc=1, device_id={"blk": (blk + i) % N_BLK}, device_id_type=MESH)

    for load in loads[3:5]:
        load.start()
    for load in loads[:3]:
        load.wait()
    for load in loads[5:]:
        load.start()
    spin_re, spin_im = spin[0], spin[1]
    leaf_sums(pos, amp, spin_re, spin_im, mom, 0)
    for load in loads[3:5]:
        load.wait()
    leaf_sums(pos, amp, spin_re, spin_im, mom, 1)
    loads[5].wait()
    local_tree(stage, mom, first_src)
    pl.semaphore_wait(barrier, 63 + N_BLK - 1)

    def first(i):
        return pltpu.make_async_remote_copy(
            src_ref=first_src.at[leaf ^ i],
            dst_ref=first_dst.at[leaf],
            send_sem=send1.at[i],
            recv_sem=recv1.at[i],
            device_id={"leaf": leaf ^ i},
            device_id_type=MESH,
        )

    def far_first(n):
        k = n // 8
        step = (k + 1) // 2
        off = (4 + step * (1 - 2 * (k % 2)) + 8) % 8
        z = (own_z + off) % 8
        return (z * 8 + n % 8) ^ leaf

    def first_send(n, carry):
        i = far_first(n)

        @pl.when(i != 0)
        def _():
            first(i).start()

        return carry

    def first_wait(i, carry):
        first(i).wait()
        return carry

    lax.fori_loop(0, 64, first_send, 0)
    first_dst[leaf] = first_src[leaf]
    loads[6].wait()
    lax.fori_loop(1, 64, first_wait, 0)
    cross_tree(stage, shift[...], first_dst, second_src)

    def near_z(c):
        k = (c + 1) // 2
        return (own_z + k * (2 * (c % 2) - 1) + 8) % 8

    def second(c, j):
        other = near_z(c) * 8 + j
        return pltpu.make_async_remote_copy(
            src_ref=second_src.at[other],
            dst_ref=roots.at[blk, leaf],
            send_sem=send2.at[other],
            recv_sem=recv2.at[leaf],
            device_id={"leaf": other},
            device_id_type=MESH,
        )

    def second_got(z, j):
        other = z * 8 + j
        return pltpu.make_async_remote_copy(
            src_ref=second_src.at[other],
            dst_ref=roots.at[blk, other],
            send_sem=send2.at[other],
            recv_sem=recv2.at[other],
            device_id={"leaf": other},
            device_id_type=MESH,
        )

    own_j = leaf % 8

    def send_own(i, carry):
        second(0, (own_j + i) % 8).start()
        return carry

    lax.fori_loop(1, 8, send_own, 0)

    def send_far(n, carry):
        second(n // 8, (own_j + n) % 8).start()
        return carry

    lax.fori_loop(8, 64, send_far, 0)
    roots[blk, leaf] = second_src[leaf]
    loads[7].wait()
    loads[8].wait()

    def third(z, i):
        return pltpu.make_async_remote_copy(
            src_ref=roots.at[blk, pl.ds(z * 8, 8)],
            dst_ref=roots.at[blk, pl.ds(z * 8, 8)],
            send_sem=send3.at[z, i],
            recv_sem=recv3.at[z, i],
            device_id={"blk": (blk + i) % N_BLK},
            device_id_type=MESH,
        )

    def third_got(z, i):
        source = (blk + N_BLK - i) % N_BLK
        return pltpu.make_async_remote_copy(
            src_ref=roots.at[blk, pl.ds(z * 8, 8)],
            dst_ref=roots.at[source, pl.ds(z * 8, 8)],
            send_sem=send3.at[z, i],
            recv_sem=recv3.at[z, i],
            device_id={"blk": (blk + i) % N_BLK},
            device_id_type=MESH,
        )

    reverse = jnp.int32(0)
    for bit in range(6):
        reverse = reverse * 2 + (leaf // 2**bit) % 2

    def chunk_step(c, carry):
        @pl.when(c < 8)
        def _():
            z = near_z(c)

            def got(j, carry):
                second_got(z, (own_j + j) % 8).wait_recv()
                return carry

            lax.fori_loop(jnp.where(c == 0, 1, 0), 8, got, 0)
            for i in (2, 1, 3):
                third(z, i).start()

        @pl.when(c >= LAG)
        def _():
            z = near_z(c - LAG)
            for i in (1, 2, 3):
                third_got(z, i).wait_recv()
            lhs, columns = coefficients(roots, z)
            fill_dense(lhs, wave, dense)
            look_up(dense, columns, tick, out, z, reverse)

        return carry

    lax.fori_loop(0, 8 + LAG, chunk_step, 0)

    def finish(z, carry):
        for i in (1, 2, 3):
            third(z, i).wait_send()
        return carry

    lax.fori_loop(0, 8, finish, 0)

    def finish_second(i, carry):
        second_got(0, leaf ^ i).wait_send()
        return carry

    lax.fori_loop(1, 64, finish_second, 0)


def local(src_pos, strengths, tgt_pos):
    stages, waves, shift, spin = tables()
    hbm = pl.BlockSpec(memory_space=pl.ANY)
    vmem, dma = pltpu.VMEM, pltpu.SemaphoreType.DMA
    f32, tiles = jnp.float32, (64, 8, 128)
    out = pl.pallas_call(
        kernel,
        out_shape=pltpu.VMEM((4096, 128), f32),
        in_specs=[hbm] * 7,
        out_specs=pl.BlockSpec(memory_space=pltpu.VMEM),
        scratch_shapes=[
            vmem((4, 2, 256, 128), jnp.int32),
            vmem((2, 4, 2, 256, 128), f32),
            vmem((2048, 128), jnp.int32),
            vmem((6, 2, 256, 256), jnp.bfloat16),
            vmem((256, 2 * HALF), jnp.bfloat16),
            vmem((2 * R, 128), f32),
            vmem((2, 8, 128), f32),
            vmem((8, 32, 256), f32),
            vmem(tiles, f32),
            vmem(tiles, f32),
            vmem(tiles, f32),
            vmem((N_BLK, *tiles), f32),
            vmem((256, 2 * HALF), jnp.int32),
            dma((9,)),
            dma((64,)),
            dma((64,)),
            dma((64,)),
            dma((64,)),
            dma((8, N_BLK)),
            dma((8, N_BLK)),
        ],
        compiler_params=pltpu.CompilerParams(collective_id=0, has_side_effects=True),
        name="butterfly",
    )(
        src_pos.reshape(4, 2, 256, 128),
        strengths.reshape(2, 4, 2, 256, 128),
        tgt_pos.reshape(2048, 128),
        jnp.asarray(stages),
        jnp.asarray(waves),
        jnp.asarray(shift),
        jnp.asarray(spin),
    )
    return jnp.transpose(out.reshape(2048, 2, 128), (1, 0, 2)).reshape(2, 2048 * 128)


def solution(mesh):
    return jax.shard_map(
        local,
        mesh=mesh,
        in_specs=(P("blk", "leaf"), P(None, "blk", "leaf"), P(("leaf", "blk"))),
        out_specs=P(None, ("leaf", "blk")),
        check_vma=False,
    )
```
